1024 devices in a mesh: row: 8 (over y), col: 128 (over z, x, core).
Axes of the slice: x: 4, y: 8, z: 16, core: 2. Of those that a mesh axis runs over, the one named last changes fastest.
Arguments:
- left_tiles: bfloat16 [2, 64, 256, 256], P(None, 'row', 'col'), may hold values from 0.02 to 3, as said below
- right_tile_store: bfloat16 [512, 48, 256, 256], P('col', 'row'), may hold values from 0.019897461 to 1
- right_index: int32 [512, 48], P('col', 'row'), may hold values from 0 to 7, as said below
- right_count: int32 [512, 8], P('col', 'row'), may hold values from 1 to 6
Outputs:
- inflated: bfloat16 [2, 512, 256, 256], P(None, 'col', 'row')
The draws below stay inside these ranges and needn't reach their ends.
Inputs may be any that keep to these rules, and one draw needn't show every extreme that they name: `right_index`: for each column block and each row index the 6 slots name distinct contraction blocks; only the first right_count of them are used. `left_tiles`: positive entries.
All inputs are finite; a program needn't handle non-finite values.
Results may differ from the reference program's by a relative error of at most 0.001.
Values may be sent and summed in bfloat16 or wider, within the bound.
A program may use at most 32 MiB of HBM per device.

```python
import math
import jax
import jax.numpy as jnp
from jax import lax

TILE_EDGE = 256
NR = 2
KR = 8
QR = 6
COLUMN_BLOCK_NUM = 512
KTOT = 64
SLOTS_PER_BLOCK = 48
N_ROW = 8


def draw_left_tiles(key, part):
    shape = (NR, KTOT, TILE_EDGE, TILE_EDGE)
    ramp = 1.0 + 2.0 * jnp.arange(TILE_EDGE, dtype=jnp.float32) / TILE_EDGE
    values = jax.random.uniform(key, shape, jnp.float32, 0.05, 1.0)
    return (values * ramp[None, None, :, None]).astype(jnp.bfloat16)


def draw_right_index(key, part):
    groups = COLUMN_BLOCK_NUM * (KTOT // KR)
    scores = jax.random.randint(key, (groups, KR), 0, 1 << 20) * KR + jnp.arange(KR)[None, :]
    order = jnp.argsort(scores, axis=1)
    return order[:, :QR].reshape(COLUMN_BLOCK_NUM, KTOT // KR * QR).astype(jnp.int32)


def touch_ends(drawn, own_key, least, largest):
    shape = drawn.shape
    index_at = [jax.random.randint(jax.random.fold_in(own_key, axis), (), 0, shape[axis]) for axis in range(len(shape))]
    drawn = drawn.at[tuple(index_at)].set(least)
    longest = shape.index(max(shape))
    index_at[longest] = (index_at[longest] + 1) % shape[longest]
    return drawn.at[tuple(index_at)].set(largest)


def level_of(key, dims, split, smallest, largest):
    gain = 1.0
    for axis_at, parts in split:
        heights = jax.random.uniform(jax.random.fold_in(jax.random.fold_in(key, 6), axis_at), (parts,), jnp.float32, smallest / len(split), largest / len(split))
        gain = gain * jnp.repeat(jnp.exp(heights), dims[axis_at] // parts).reshape((-1,) + (1,) * (len(dims) - 1 - axis_at))
    return gain


def setup_inputs(seed: int = 0) -> dict:
    streams_of = jax.random.split(jax.random.key(seed), 5)
    left_tiles = draw_left_tiles(jax.random.fold_in(streams_of[4], 71), 0)
    right_tile_store = jnp.clip(jnp.exp(math.log(1.0) - 3.9171631 * jax.random.uniform(streams_of[1], (COLUMN_BLOCK_NUM, SLOTS_PER_BLOCK, TILE_EDGE, TILE_EDGE), jnp.float32) ** level_of(streams_of[1], (COLUMN_BLOCK_NUM, SLOTS_PER_BLOCK, TILE_EDGE, TILE_EDGE), ((0, 128), (1, 8)), -0.2, 0.2)), 0.019897461, 1.0).astype(jnp.bfloat16)
    right_index = draw_right_index(jax.random.fold_in(streams_of[4], 71), 0)
    right_count = touch_ends(jax.random.randint(streams_of[3], (COLUMN_BLOCK_NUM, N_ROW), 1, QR + 1), jax.random.fold_in(streams_of[3], 1), 1, QR).astype(jnp.int32)
    return {"left_tiles": left_tiles, "right_tile_store": right_tile_store, "right_index": right_index, "right_count": right_count}


def reference(left_tiles, right_tile_store, right_index, right_count):
    row_grouping = right_count.shape[1]
    slot_total = right_tile_store.shape[1] // row_grouping
    block_count = left_tiles.shape[1] // row_grouping
    window_blocks = left_tiles.shape[0]
    tile_size = left_tiles.shape[2]

    def single_column(inputs):
        tiles, index, counts = inputs
        offsets = (jnp.arange(row_grouping, dtype=jnp.int32) * block_count).astype(jnp.int32)
        global_index = (index.reshape(row_grouping, slot_total).astype(jnp.int32) + offsets[:, None]).astype(jnp.int32)
        picked = jnp.take(left_tiles, global_index.reshape(-1), axis=1)
        live_mask = (jnp.arange(slot_total, dtype=jnp.int32)[None, :] < counts[:, None]).reshape(-1)
        picked = picked * live_mask.astype(left_tiles.dtype)[None, :, None, None]
        picked = picked.reshape(window_blocks, row_grouping, slot_total, tile_size, tile_size)
        grouped_tiles = tiles.reshape(row_grouping, slot_total, tile_size, tile_size)
        partial_value = jnp.einsum("arqmb,rqbn->armn", picked.astype(jnp.float32), grouped_tiles.astype(jnp.float32))
        return jnp.sum(partial_value, axis=1)

    product = lax.map(single_column, (right_tile_store, right_index, right_count))
    squared = product * product
    column_sums = jnp.sum(squared, axis=(1, 2))
    scaled = squared * ((window_blocks * tile_size) / column_sums[:, None, None, :])
    return jnp.transpose(scaled, (1, 0, 2, 3)).astype(jnp.bfloat16)
```

```python
import math

import jax
import jax.numpy as jnp
from jax import lax
from jax.experimental import pallas as pl
from jax.experimental.pallas import tpu as pltpu
from jax.sharding import Mesh
from jax.sharding import PartitionSpec as P

COL = ("col_0", "col_1", "col_2")
AXES = ("row", *COL)

Y, Z, X, C = 8, 16, 4, 2
REACH = 4
SLOTS_1 = 2 * REACH + 1
SLOTS_2 = Z - SLOTS_1

LOW, HIGH = math.log(0.1), math.log(40000.0)
CENTRE = (LOW + HIGH) / 2
STEP = (HIGH - LOW) / 65000


def encode(value):
    scaled = (jnp.log(value) - CENTRE) * (1 / STEP)
    return jnp.round(scaled).astype(jnp.int32).astype(jnp.int16)


def decode(code):
    return jnp.exp(code.astype(jnp.int32).astype(jnp.float32) * STEP + CENTRE)


def kernel(
    index_ref, count_ref, left_ref, right_hbm, out_ref,
    right, parts, rows, partial, sent, got, sums, sums_in,
    load_sem, z_sem, x_sem, core_sem, row_sem, sums_sem, send_sem,
):
    y, z, x, c = (lax.axis_index(name) for name in AXES)
    blocks, slots, edge = right_hbm.shape[0], right_hbm.shape[1], right_hbm.shape[2]
    window, kr = left_ref.shape[0], left_ref.shape[1]
    share = edge // Y
    piece = parts.shape[1]

    def at(dy=0, dz=0, dx=0, dc=0):
        return (
            lax.rem(y + dy + Y, Y),
            lax.rem(z + dz + Z, Z),
            lax.rem(x + dx + X, X),
            lax.rem(c + dc, C),
        )

    loads = [
        pltpu.make_async_copy(right_hbm.at[j], right.at[j], load_sem.at[j])
        for j in range(blocks)
    ]
    for load in loads:
        load.start()

    peers = [at(dz=d) for d in range(-REACH, REACH + 1) if d]
    peers += [at(dx=1), at(dx=-1), at(dc=1)]
    peers += [at(dy=d) for d in range(1, Y)]
    barrier = pltpu.get_barrier_semaphore()
    for peer in peers:
        pl.semaphore_signal(barrier, inc=1, device_id=peer, device_id_type=pl.DeviceIdType.MESH)

    def base(dx, dc=0):
        return (lax.rem(x + dx + X, X) * C + lax.rem(c + dc, C)) * Z

    mine = base(0)
    parts[mine + REACH] = left_ref[...].reshape(piece, edge)
    rows[:, kr] = jnp.zeros((window, edge, edge), jnp.bfloat16)
    pl.semaphore_wait(barrier, len(peers))

    def copy(src, dst, recv, to, kind=0):
        return pltpu.make_async_remote_copy(
            src_ref=src, dst_ref=dst, send_sem=send_sem.at[kind], recv_sem=recv,
            device_id=to, device_id_type=pl.DeviceIdType.MESH,
        )

    def pass_on(first, number, recv, to):
        where = parts.at[pl.ds(first, number)]
        copy(where, where, recv, to).start()

    def arrived(number, recv):
        where = parts.at[pl.ds(0, number)]
        pltpu.make_async_copy(where, where, recv).wait()

    own = parts.at[mine + REACH]
    for d in range(REACH, 0, -1):
        far = d == REACH
        copy(own, parts.at[mine + REACH - d], z_sem.at[0 if far else 2], at(dz=d)).start()
        copy(own, parts.at[mine + REACH + d], z_sem.at[1 if far else 2], at(dz=-d)).start()
    arrived(1, z_sem.at[0])
    for d in range(REACH, 0, -1):
        copy(parts.at[mine], parts.at[mine + Z - d], z_sem.at[3], at(dz=d)).start()
    arrived(1, z_sem.at[1])
    for d in range(REACH - 1, 0, -1):
        copy(
            parts.at[mine + 2 * REACH], parts.at[mine + 2 * REACH + d], z_sem.at[3], at(dz=-d)
        ).start()

    batches = ((0, SLOTS_1), (SLOTS_1, SLOTS_2))

    def to_core(b, way, dx):
        first, number = batches[b]
        pass_on(base(dx) + first, number, core_sem.at[b, way], at(dc=1))

    def near(b):
        first, number = batches[b]
        pass_on(mine + first, number, x_sem.at[b, 0], at(dx=1))
        pass_on(mine + first, number, x_sem.at[b, 1], at(dx=-1))
        to_core(b, 0, 0)

    def across(b):
        first, number = batches[b]
        half = number // 2
        arrived(number, x_sem.at[b, 0])
        pass_on(base(-1) + first, half, x_sem.at[b, 2], at(dx=1))
        arrived(number, x_sem.at[b, 1])
        pass_on(base(1) + first + half, number - half, x_sem.at[b, 3], at(dx=-1))
        to_core(b, 1, -1)
        to_core(b, 2, 1)

    def last(b):
        first, number = batches[b]
        half = number // 2
        arrived(half, x_sem.at[b, 2])
        arrived(number - half, x_sem.at[b, 3])
        to_core(b, 3, 2)

    out_row = lax.broadcasted_iota(jnp.int32, (edge, edge), 0)
    in_row = lax.broadcasted_iota(jnp.int32, (edge, edge), 1)
    per = piece // (window * kr)
    span = per * X * C
    tile, within = lax.div(out_row, span), lax.rem(out_row, span)
    source = lax.div(within, per) * piece + tile * per + lax.rem(within, per)
    order = (source == in_row).astype(jnp.float32).astype(jnp.bfloat16)

    def spread(b):
        first, number = batches[b]
        for way in range(4):
            arrived(number, core_sem.at[b, way])

        def one(slot, carry):
            mixed = jnp.concatenate([parts[d * Z + slot] for d in range(X * C)], axis=0)
            placed = jnp.dot(order, mixed, preferred_element_type=jnp.float32)
            placed = placed.astype(jnp.bfloat16).reshape(window, kr, span, edge)
            start = pl.multiple_of(lax.rem(z + slot + Z - REACH, Z) * span, span)
            rows[:, pl.ds(0, kr), pl.ds(start, span), :] = placed
            return carry

        lax.fori_loop(first, first + number, one, 0)

    arrived(2 * REACH - 2, z_sem.at[2])
    near(0)
    across(0)
    arrived(SLOTS_2, z_sem.at[3])
    near(1)
    last(0)
    across(1)
    spread(0)
    last(1)
    for load in loads:
        load.wait()
    spread(1)

    def multiply(slot, dy):
        start = pl.multiple_of(lax.rem(y + dy + Y, Y) * share, share)

        def one(j, carry):
            live = count_ref[j, 0]
            picked = []
            for q in range(slots):
                k = jnp.where(q < live, index_ref[j, q], kr)
                picked.append(rows[:, k, pl.ds(start, share), :].reshape(window * share, edge))
            partial[slot, j] = jnp.dot(
                jnp.concatenate(picked, axis=1),
                right[j].reshape(slots * edge, edge),
                preferred_element_type=jnp.float32,
            )
            return carry

        lax.fori_loop(0, blocks, one, 0)

    half = blocks // 2
    far = Y // 2

    def message(step, way, j):
        return (step * 2 + way) * blocks + j

    def pass_sum(step, way, j, add):
        slot = 0 if step == 0 else way
        value = partial[slot, j]
        if add:
            wait_sum(step - 1, way, j)
            value = value + decode(got[message(step - 1, way, j)])
        n = message(step, way, j)
        place = n - (way if step == 0 else 1) * blocks
        sent[place] = encode(value)
        copy(sent.at[place], got.at[n], row_sem.at[n], at(dy=1 if way == 0 else -1), 1).start()

    def wait_sum(step, way, j):
        n = message(step, way, j)
        pltpu.make_async_copy(got.at[n], got.at[n], row_sem.at[n]).wait()

    def each(first, last_one, body):
        def one(j, carry):
            body(j)
            return carry

        lax.fori_loop(first, last_one, one, 0)

    multiply(0, far)
    each(0, half, lambda j: pass_sum(0, 0, j, False))
    each(half, blocks, lambda j: pass_sum(0, 1, j, False))
    for step in range(1, far):
        multiply(0, far - step)
        multiply(1, step - far)
        if step == 1:
            each(half, blocks, lambda j: pass_sum(1, 0, j, False))
            each(0, half, lambda j: pass_sum(1, 1, j, False))
            each(0, half, lambda j: pass_sum(1, 0, j, True))
            each(half, blocks, lambda j: pass_sum(1, 1, j, True))
        else:
            def both(j, step=step):
                pass_sum(step, 0, j, True)
                pass_sum(step, 1, j, True)

            each(0, blocks, both)
    multiply(0, 0)
    for j in range(blocks):
        wait_sum(far - 1, 0, j)
        wait_sum(far - 1, 1, j)
        product = (
            partial[0, j]
            + decode(got[message(far - 1, 0, j)])
            + decode(got[message(far - 1, 1, j)])
        )
        squared = product * product
        partial[1, j] = squared
        sums[j : j + 1, :] = jnp.sum(squared, axis=0, keepdims=True)
    for d in range(1, Y):
        copy(sums, sums_in.at[d - 1], sums_sem.at[0], at(dy=d), 2).start()
    pltpu.make_async_copy(sums_in, sums_in, sums_sem.at[0]).wait()
    total = sums[...]
    for d in range(Y - 1):
        total = total + sums_in[d]
    scale = (window * edge) / total
    for j in range(blocks):
        scaled = partial[1, j] * scale[j : j + 1, :]
        out_ref[:, j] = scaled.astype(jnp.bfloat16).reshape(window, share, edge)

    for kind, whole in enumerate((parts.at[pl.ds(0, X * C * Z - 1)], sent, sums_in)):
        pltpu.make_async_copy(whole, whole, send_sem.at[kind]).wait()


def shards(left_tiles, right_tile_store, right_index, right_count):
    window, kr, per, edge = left_tiles.shape
    blocks, slots = right_tile_store.shape[:2]
    share = edge // Y
    piece = window * kr * per
    messages = (Y // 2) * 2 * blocks
    return pl.pallas_call(
        kernel,
        out_shape=jax.ShapeDtypeStruct((window, blocks, share, edge), jnp.bfloat16),
        in_specs=[
            pl.BlockSpec(memory_space=pltpu.SMEM),
            pl.BlockSpec(memory_space=pltpu.SMEM),
            pl.BlockSpec(memory_space=pltpu.VMEM),
            pl.BlockSpec(memory_space=pl.ANY),
        ],
        out_specs=pl.BlockSpec(memory_space=pltpu.VMEM),
        scratch_shapes=[
            pltpu.VMEM((blocks, slots, edge, edge), jnp.bfloat16),
            pltpu.VMEM((X * C * Z, piece, edge), jnp.bfloat16),
            pltpu.VMEM((window, kr + 1, edge, edge), jnp.bfloat16),
            pltpu.VMEM((2, blocks, window * share, edge), jnp.float32),
            pltpu.VMEM((messages - blocks, window * share, edge), jnp.int16),
            pltpu.VMEM((messages, window * share, edge), jnp.int16),
            pltpu.VMEM((blocks, edge), jnp.float32),
            pltpu.VMEM((Y - 1, blocks, edge), jnp.float32),
            pltpu.SemaphoreType.DMA((blocks,)),
            pltpu.SemaphoreType.DMA((4,)),
            pltpu.SemaphoreType.DMA((2, 4)),
            pltpu.SemaphoreType.DMA((2, 4)),
            pltpu.SemaphoreType.DMA((messages,)),
            pltpu.SemaphoreType.DMA((1,)),
            pltpu.SemaphoreType.DMA((3,)),
        ],
        compiler_params=pltpu.CompilerParams(
            collective_id=0, has_side_effects=True, vmem_limit_bytes=48 * 1024 * 1024
        ),
    )(right_index, right_count, left_tiles, right_tile_store)


def solution(mesh):
    split = Mesh(mesh.devices.reshape(Y, Z, X, C), AXES)
    return jax.shard_map(
        shards,
        mesh=split,
        in_specs=(
            P(None, "row", COL, None),
            P(COL, "row", None, None),
            P(COL, "row"),
            P(COL, "row"),
        ),
        out_specs=P(None, COL, "row", None),
        check_vma=False,
    )
```

```python
import math

import jax
import jax.numpy as jnp
from jax import lax
from jax.experimental import pallas as pl
from jax.experimental.pallas import tpu as pltpu
from jax.sharding import Mesh
from jax.sharding import PartitionSpec as P

COL = ("col_0", "col_1", "col_2")
AXES = ("row", *COL)

Y, Z, X, C = 8, 16, 4, 2
REACH = 4
SLOTS_1 = 2 * REACH + 1
SLOTS_2 = Z - SLOTS_1

LOW, HIGH = math.log(0.1), math.log(40000.0)
CENTRE = (LOW + HIGH) / 2
STEP = (HIGH - LOW) / 65000


def encode(value):
    scaled = (jnp.log(value) - CENTRE) * (1 / STEP)
    return jnp.round(scaled).astype(jnp.int32).astype(jnp.int16)


def decode(code):
    return jnp.exp(code.astype(jnp.int32).astype(jnp.float32) * STEP + CENTRE)


def kernel(
    index_hbm, count_hbm, left_hbm, right_hbm, out_ref,
    index_ref, count_ref, left_ref, right, parts, rows, partial, sent, got, sums, sums_in,
    load_sem, small_sem, z_sem, x_sem, core_sem, row_sem, sums_sem, send_sem,
):
    y, z, x, c = (lax.axis_index(name) for name in AXES)
    blocks, slots, edge = right_hbm.shape[0], right_hbm.shape[1], right_hbm.shape[2]
    window, kr = left_ref.shape[0], left_ref.shape[1]
    share = edge // Y
    piece = parts.shape[2]

    def at(dy=0, dz=0, dx=0, dc=0):
        return (
            lax.rem(y + dy + Y, Y),
            lax.rem(z + dz + Z, Z),
            lax.rem(x + dx + X, X),
            lax.rem(c + dc, C),
        )

    loads = [
        pltpu.make_async_copy(right_hbm.at[j], right.at[j], load_sem.at[j])
        for j in range(blocks)
    ]
    small = [
        pltpu.make_async_copy(src, dst, small_sem.at[n])
        for n, (src, dst) in enumerate(
            ((left_hbm, left_ref), (index_hbm, index_ref), (count_hbm, count_ref))
        )
    ]
    for load in small + loads:
        load.start()

    peers = [at(dz=d) for d in range(-REACH, REACH + 1) if d]
    peers += [at(dx=1), at(dx=-1), at(dc=1)]
    peers += [at(dy=d) for d in range(1, Y)]
    barrier = pltpu.get_barrier_semaphore()
    for peer in peers:
        pl.semaphore_signal(barrier, inc=1, device_id=peer, device_id_type=pl.DeviceIdType.MESH)

    def base(dx, dc=0):
        return (lax.rem(x + dx + X, X) * C + lax.rem(c + dc, C)) * Z

    mine = base(0)
    small[0].wait()
    for w in range(window):
        parts[w, mine + REACH] = left_ref[w].reshape(piece, edge)
    rows[:, kr] = jnp.zeros((window, edge, edge), jnp.bfloat16)

    per = piece // kr
    span = per * X * C
    out_row = lax.broadcasted_iota(jnp.int32, (kr * span, kr * span), 0)
    in_row = lax.broadcasted_iota(jnp.int32, (kr * span, kr * span), 1)
    tile, within = lax.div(out_row, span), lax.rem(out_row, span)
    source = lax.div(within, per) * piece + tile * per + lax.rem(within, per)
    order = (source == in_row).astype(jnp.float32).astype(jnp.bfloat16)
    pl.semaphore_wait(barrier, len(peers))

    def copy(src, dst, recv, to, kind):
        return pltpu.make_async_remote_copy(
            src_ref=src, dst_ref=dst, send_sem=send_sem.at[kind], recv_sem=recv,
            device_id=to, device_id_type=pl.DeviceIdType.MESH,
        )

    def pass_on(w, first, number, recv, to):
        where = parts.at[w, pl.ds(first, number)]
        copy(where, where, recv, to, w).start()

    def arrived(number, recv):
        where = parts.at[0, pl.ds(0, number)]
        pltpu.make_async_copy(where, where, recv).wait()

    def start_z(w):
        own = parts.at[w, mine + REACH]
        for d in range(REACH, 0, -1):
            far = d == REACH
            up = parts.at[w, mine + REACH - d]
            down = parts.at[w, mine + REACH + d]
            copy(own, up, z_sem.at[w, 0 if far else 2], at(dz=d), w).start()
            copy(own, down, z_sem.at[w, 1 if far else 2], at(dz=-d), w).start()

    def relay_z(w):
        low, high = parts.at[w, mine], parts.at[w, mine + 2 * REACH]
        arrived(1, z_sem.at[w, 0])
        for d in range(REACH, 0, -1):
            copy(low, parts.at[w, mine + Z - d], z_sem.at[w, 3], at(dz=d), w).start()
        arrived(1, z_sem.at[w, 1])
        for d in range(REACH - 1, 0, -1):
            to = parts.at[w, mine + 2 * REACH + d]
            copy(high, to, z_sem.at[w, 3], at(dz=-d), w).start()

    batches = ((0, SLOTS_1), (SLOTS_1, SLOTS_2))

    def to_core(w, b, way, dx):
        first, number = batches[b]
        pass_on(w, base(dx) + first, number, core_sem.at[w, b, way], at(dc=1))

    def near(w, b):
        first, number = batches[b]
        arrived(2 * REACH - 2 if b == 0 else SLOTS_2, z_sem.at[w, 2 + b])
        pass_on(w, mine + first, number, x_sem.at[w, b, 0], at(dx=1))
        pass_on(w, mine + first, number, x_sem.at[w, b, 1], at(dx=-1))
        to_core(w, b, 0, 0)

    def across(w, b):
        first, number = batches[b]
        half = number // 2
        arrived(number, x_sem.at[w, b, 0])
        pass_on(w, base(-1) + first, half, x_sem.at[w, b, 2], at(dx=1))
        arrived(number, x_sem.at[w, b, 1])
        pass_on(w, base(1) + first + half, number - half, x_sem.at[w, b, 3], at(dx=-1))
        to_core(w, b, 1, -1)
        to_core(w, b, 2, 1)

    def last(w, b):
        first, number = batches[b]
        half = number // 2
        arrived(half, x_sem.at[w, b, 2])
        arrived(number - half, x_sem.at[w, b, 3])
        to_core(w, b, 3, 2)

    def spread(w, b):
        first, number = batches[b]
        for way in range(4):
            arrived(number, core_sem.at[w, b, way])

        def one(slot, carry):
            mixed = jnp.concatenate([parts[w, d * Z + slot] for d in range(X * C)], axis=0)
            placed = jnp.dot(order, mixed, preferred_element_type=jnp.float32)
            placed = placed.astype(jnp.bfloat16).reshape(kr, span, edge)
            start = pl.multiple_of(lax.rem(z + slot + Z - REACH, Z) * span, span)
            rows[w, pl.ds(0, kr), pl.ds(start, span), :] = placed
            return carry

        lax.fori_loop(first, first + number, one, 0)

    half = blocks // 2
    far = Y // 2

    def each(first, last_one, body):
        def one(j, carry):
            body(j)
            return carry

        lax.fori_loop(first, last_one, one, 0)

    def multiply(w, *targets):
        starts = [pl.multiple_of(lax.rem(y + dy + Y, Y) * share, share) for dy in targets]

        def one(j):
            live = count_ref[0, j]
            picked = []
            for q in range(slots):
                k = jnp.where(q < live, index_ref[j, q], kr)
                picked.append(
                    jnp.concatenate([rows[w, k, pl.ds(at, share), :] for at in starts], axis=0)
                )
            result = jnp.dot(
                jnp.concatenate(picked, axis=1),
                right[j].reshape(slots * edge, edge),
                preferred_element_type=jnp.float32,
            )
            for slot in range(len(starts)):
                partial[w, slot, j] = result[slot * share : (slot + 1) * share]

        each(0, blocks, one)

    def message(step, way, j):
        return (step * 2 + way) * blocks + j

    def wait_sum(w, step, way, j):
        n = message(step, way, j)
        pltpu.make_async_copy(got.at[w, n], got.at[w, n], row_sem.at[w, n]).wait()

    def pass_sum(w, step, way, j, add):
        value = partial[w, 0 if step == 0 else way, j]
        if add:
            wait_sum(w, step - 1, way, j)
            value = value + decode(got[w, message(step - 1, way, j)])
        n = message(step, way, j)
        place = n - (way if step == 0 else 1) * blocks
        sent[w, place] = encode(value)
        to = at(dy=1 if way == 0 else -1)
        copy(sent.at[w, place], got.at[w, n], row_sem.at[w, n], to, 2).start()

    def first_sums(w):
        multiply(w, far)
        each(0, half, lambda j: pass_sum(w, 0, 0, j, False))
        each(half, blocks, lambda j: pass_sum(w, 0, 1, j, False))

    def second_sums(w):
        multiply(w, far - 1, 1 - far)
        each(half, blocks, lambda j: pass_sum(w, 1, 0, j, False))
        each(0, half, lambda j: pass_sum(w, 1, 1, j, False))

    def next_sums(w, step):
        if step == 1:
            def both(j):
                pass_sum(w, 1, 0, j, True)
                pass_sum(w, 1, 1, j + half, True)

            each(0, half, both)
        else:
            def both(j):
                pass_sum(w, step, 0, j, True)
                pass_sum(w, step, 1, j, True)

            each(0, blocks, both)
        left = far - step - 1
        multiply(w, *((left, -left) if left else (0,)))

    for w in range(window):
        start_z(w)
    for w in range(window):
        relay_z(w)
    for w in range(window):
        near(w, 0)
    for load in small[1:] + loads:
        load.wait()
    for w in range(window):
        across(w, 0)
    for w in range(window):
        near(w, 1)
    for w in range(window):
        last(w, 0)
    spread(0, 0)
    across(0, 1)
    spread(1, 0)
    across(1, 1)
    last(0, 1)
    last(1, 1)
    spread(0, 1)
    first_sums(0)
    spread(1, 1)
    first_sums(1)
    for w in range(window):
        second_sums(w)
    for step in range(1, far):
        for w in range(window):
            next_sums(w, step)

    for w in range(window):
        for j in range(blocks):
            wait_sum(w, far - 1, 0, j)
            wait_sum(w, far - 1, 1, j)
            product = (
                partial[w, 0, j]
                + decode(got[w, message(far - 1, 0, j)])
                + decode(got[w, message(far - 1, 1, j)])
            )
            squared = product * product
            partial[w, 1, j] = squared
            column = jnp.sum(squared, axis=0, keepdims=True)
            sums[j : j + 1, :] = column if w == 0 else sums[j : j + 1, :] + column
    for d in range(1, Y):
        copy(sums, sums_in.at[d - 1], sums_sem.at[0], at(dy=d), 3).start()
    pltpu.make_async_copy(sums_in, sums_in, sums_sem.at[0]).wait()
    total = sums[...]
    for d in range(Y - 1):
        total = total + sums_in[d]
    scale = (window * edge) / total
    for j in range(blocks):
        for w in range(window):
            out_ref[w, j] = (partial[w, 1, j] * scale[j : j + 1, :]).astype(jnp.bfloat16)

    for w in range(window):
        moved = parts.at[w, pl.ds(0, X * C * Z - 1)]
        pltpu.make_async_copy(moved, moved, send_sem.at[w]).wait()
    pltpu.make_async_copy(sent, sent, send_sem.at[2]).wait()
    pltpu.make_async_copy(sums_in, sums_in, send_sem.at[3]).wait()


def shards(left_tiles, right_tile_store, right_index, right_count):
    window, kr, per, edge = left_tiles.shape
    blocks, slots = right_tile_store.shape[:2]
    share = edge // Y
    piece = kr * per
    messages = (Y // 2) * 2 * blocks
    return pl.pallas_call(
        kernel,
        out_shape=jax.ShapeDtypeStruct((window, blocks, share, edge), jnp.bfloat16),
        in_specs=[
            pl.BlockSpec(memory_space=pltpu.HBM),
            pl.BlockSpec(memory_space=pltpu.HBM),
            pl.BlockSpec(memory_space=pltpu.HBM),
            pl.BlockSpec(memory_space=pltpu.HBM),
        ],
        out_specs=pl.BlockSpec(memory_space=pltpu.VMEM),
        scratch_shapes=[
            pltpu.SMEM((blocks, slots), jnp.int32),
            pltpu.SMEM((1, blocks), jnp.int32),
            pltpu.VMEM((window, kr, per, edge), jnp.bfloat16),
            pltpu.VMEM((blocks, slots, edge, edge), jnp.bfloat16),
            pltpu.VMEM((window, X * C * Z, piece, edge), jnp.bfloat16),
            pltpu.VMEM((window, kr + 1, edge, edge), jnp.bfloat16),
            pltpu.VMEM((window, 2, blocks, share, edge), jnp.float32),
            pltpu.VMEM((window, messages - blocks, share, edge), jnp.int16),
            pltpu.VMEM((window, messages, share, edge), jnp.int16),
            pltpu.VMEM((blocks, edge), jnp.float32),
            pltpu.VMEM((Y - 1, blocks, edge), jnp.float32),
            pltpu.SemaphoreType.DMA((blocks,)),
            pltpu.SemaphoreType.DMA((3,)),
            pltpu.SemaphoreType.DMA((window, 4)),
            pltpu.SemaphoreType.DMA((window, 2, 4)),
            pltpu.SemaphoreType.DMA((window, 2, 4)),
            pltpu.SemaphoreType.DMA((window, messages)),
            pltpu.SemaphoreType.DMA((1,)),
            pltpu.SemaphoreType.DMA((4,)),
        ],
        compiler_params=pltpu.CompilerParams(
            collective_id=0, has_side_effects=True, vmem_limit_bytes=67_043_328
        ),
    )(right_index, right_count.T, left_tiles, right_tile_store)


def solution(mesh):
    split = Mesh(mesh.devices.reshape(Y, Z, X, C), AXES)
    return jax.shard_map(
        shards,
        mesh=split,
        in_specs=(
            P(None, "row", COL, None),
            P(COL, "row", None, None),
            P(COL, "row"),
            P(COL, "row"),
        ),
        out_specs=P(None, COL, "row", None),
        check_vma=False,
    )
```
